32 devices in a mesh: fsdp: 4 (over y, core), sp: 8 (over z, x).
Axes of the slice: x: 2, y: 2, z: 4, core: 2. Of those that a mesh axis runs over, the one named last changes fastest.
Arguments:
- hidden: bfloat16 [4, 2048, 5120], P('fsdp', 'sp'), may hold values from -6 to 6
- queries: bfloat16 [4, 2048, 4096], P('fsdp', 'sp'), may hold values from -240 to 240
- norm_gain: float32 [5120], replicated, may hold values from 0.5 to 1.5
- kv_weight: bfloat16 [5120, 2048], P('fsdp'), may hold values from -0.078125 to 0.078125
- value_bias: float32 [1024], replicated, may hold values from -3 to 3
- doc_lengths: int32 [4, 16], P('fsdp'), may hold values from 1 to 512, 2048 in all within a row
Outputs:
- attended: bfloat16 [4, 2048, 4096], P('fsdp', 'sp')
The draws below stay inside these ranges and needn't reach their ends.
Inputs may be any that keep to these rules, and one draw needn't show every extreme that they name: `doc_lengths`: each row sums to 2048 and its largest entry is 512.
All inputs are finite; a program needn't handle non-finite values.
Results may differ from the reference program's by a relative error of at most 0.0067.
Values may be sent and summed in bfloat16 or wider, within the bound.
A program may use at most 128 MiB of HBM per device.

```python
import math
import jax
import jax.numpy as jnp
import numpy as np
from jax import lax

D = 5120
QH = 32
KVH = 8
HD = 128
NDOC = 16
GROUPS = 4
SEQ = 2048
MOST = 512


def draw_queries(key, part):
    drawn = jnp.clip(jax.random.normal(key, (GROUPS, SEQ, QH * HD), jnp.float32), -6.0, 6.0)
    return drawn.astype(jnp.bfloat16)


def steps_of(rng, extent, shards, low, high):
    loudness, own = 1.0, jax.random.fold_in(rng, 6)
    for position, parts in shards:
        steps = jnp.exp(jax.random.uniform(jax.random.fold_in(own, position), (parts,), jnp.float32, low / len(shards), high / len(shards)))
        loudness = loudness * jnp.repeat(steps, extent[position] // parts).reshape([-1 if axis == position else 1 for axis in range(len(extent))])
    return loudness


def split_up(number_of, total, bound, lean):
    portions = [(1 << 20) // math.isqrt(standing ** lean) + 1 for standing in range(2, number_of + 1)]
    spare, given = total - bound - (number_of - 1), [1] * (number_of - 1)
    while spare > 0:
        movable = [i for i in range(number_of - 1) if given[i] < bound]
        whole, remaining = sum([portions[i] for i in movable]), spare
        for i in movable:
            addition = min(bound - given[i], max(1, remaining * portions[i] // whole), spare)
            given[i] = given[i] + addition
            spare = spare - addition
    return np.array([bound] + given)


def uneven(key, count, total, reach, skew):
    if count == 2:
        one = jax.random.randint(key, (), max(1, total - reach), min(reach, total - 1) + 1)
        return jnp.stack([one, total - one])
    sizes = jnp.asarray(split_up(count, total, reach, skew), jnp.int32)
    couples = (count - 1) // 2
    donor, taker = sizes[1:1 + 2 * couples:2], sizes[2:2 + 2 * couples:2]
    room = jnp.minimum(donor - 1, reach - taker)
    shifted = jax.random.randint(jax.random.fold_in(key, 1), (couples,), 0, 1 << 20) % (room + 1)
    sizes = sizes.at[1:1 + 2 * couples:2].set(donor - shifted).at[2:2 + 2 * couples:2].set(taker + shifted)
    return sizes[jax.random.permutation(jax.random.fold_in(key, 2), count)]


def gaussian(key, shape, width, most, cuts=(), kind=jnp.bfloat16):
    values = jax.random.normal(key, shape, jnp.float32) * width
    if len(cuts) > 0:
        values = steps_of(key, shape, cuts, -0.22, 0.18) * values
    return jnp.clip(values, min=-most, max=most).astype(kind)


def setup_inputs(seed: int = 0) -> dict:
    seeds = jax.random.split(jax.random.key(seed), 7)
    hidden = gaussian(seeds[0], (GROUPS, SEQ, D), 1.0, 6.0, ((0, 4), (1, 8)))
    queries = draw_queries(jax.random.fold_in(seeds[6], 71), 0)
    norm_gain = jnp.clip(1.0 + 0.1 * jax.random.normal(seeds[2], (D,), jnp.float32), 0.5, 1.5)
    kv_weight = gaussian(seeds[3], (D, 2 * KVH * HD), D ** -0.5, 0.078125, ((0, 4),))
    value_bias = gaussian(seeds[4], (KVH * HD,), 0.5, 3.0, (), jnp.float32)
    doc_lengths = jax.vmap(lambda own: uneven(own, NDOC, SEQ, MOST, 2))(jax.random.split(seeds[5], GROUPS)).reshape((GROUPS, NDOC)).astype(jnp.int32)
    return {"hidden": hidden, "queries": queries, "norm_gain": norm_gain, "kv_weight": kv_weight, "value_bias": value_bias, "doc_lengths": doc_lengths}


EPS = 1e-06

def attend(query_all, key_all, value_all, doc_ids):
    length = query_all.shape[0]
    block = min(512, length)
    longest = length // 4
    window = min(length, block + longest)
    scale = HD ** (-0.5)

    def one_block(index):
        first = (index * block).astype(jnp.int32)
        start = jnp.clip(first - longest, 0, length - window).astype(jnp.int32)
        query_block = lax.dynamic_slice_in_dim(query_all, first, block, 0).astype(jnp.float32)
        key_block = lax.dynamic_slice_in_dim(key_all, start, window, 0).astype(jnp.float32)
        value_block = lax.dynamic_slice_in_dim(value_all, start, window, 0).astype(jnp.float32)
        query_ids = lax.dynamic_slice_in_dim(doc_ids, first, block, 0)
        key_ids = lax.dynamic_slice_in_dim(doc_ids, start, window, 0)
        query_pos = first + jnp.arange(block, dtype=jnp.int32)
        key_pos = start + jnp.arange(window, dtype=jnp.int32)
        allowed = (key_pos[None, :] <= query_pos[:, None]) & (key_ids[None, :] == query_ids[:, None])
        scores = jnp.einsum('qnd,knd->nqk', query_block, key_block) * scale
        scores = jnp.where(allowed[None], scores, -jnp.inf)
        highest = lax.optimization_barrier(jnp.max(scores, axis=-1, keepdims=True))
        probs = jnp.exp(scores - highest)
        probs = (probs / lax.optimization_barrier(jnp.sum(probs, axis=-1, keepdims=True))).astype(jnp.bfloat16)
        output = jnp.einsum('nqk,knd->qnd', probs.astype(jnp.float32), value_block)
        return output.astype(jnp.bfloat16)
    blocks = lax.map(one_block, jnp.arange(length // block, dtype=jnp.int32))
    return blocks.reshape(length, query_all.shape[1], query_all.shape[2])

def reference(hidden, queries, norm_gain, kv_weight, value_bias, doc_lengths):
    wide = hidden.astype(jnp.float32)
    normed = (wide * lax.rsqrt(lax.optimization_barrier(jnp.mean(wide * wide, axis=-1, keepdims=True)) + EPS) * norm_gain).astype(jnp.bfloat16)
    projected = jnp.dot(normed.reshape(GROUPS * SEQ, D), kv_weight, preferred_element_type=jnp.float32)
    projected = projected.reshape(GROUPS, SEQ, 2 * KVH * HD)
    keys = projected[..., :KVH * HD].astype(jnp.bfloat16)
    values = (projected[..., KVH * HD:] + value_bias).astype(jnp.bfloat16)
    ratio = QH // KVH

    def one_group(operands):
        query_group, key_group, value_group, lengths = operands
        ends = jnp.cumsum(lengths).astype(jnp.int32)
        positions = jnp.arange(SEQ, dtype=jnp.int32)
        doc_ids = lax.optimization_barrier(jnp.sum((positions[:, None] >= ends[None, :]).astype(jnp.int32), axis=1)).astype(jnp.int32)
        query_heads = query_group.reshape(SEQ, QH, HD)
        key_heads = jnp.repeat(key_group.reshape(SEQ, KVH, HD), ratio, axis=1)
        value_heads = jnp.repeat(value_group.reshape(SEQ, KVH, HD), ratio, axis=1)
        return attend(query_heads, key_heads, value_heads, doc_ids).reshape(SEQ, QH * HD)
    return lax.map(one_group, (queries, keys, values, doc_lengths))
```

```python
import functools
import math

import jax
import jax.numpy as jnp
from jax import lax
from jax.experimental import pallas as pl
from jax.experimental.pallas import tpu as pltpu
from jax.sharding import PartitionSpec as P

QH = 32
KVH = 8
HD = 128
EPS = 1e-06
PAIR = 2 * HD
PAIRS = KVH // 2
MSGS = 2 * KVH
LAST = MSGS - 2
SEATS = MSGS + 2
XCH = 8
QB = 128
MASKED = -1e30


def kernel(
    n, s, reach,
    x_hbm, q_hbm, gain_hbm, w_hbm, vbias_hbm, docs_hbm,
    out,
    docs, x, q, gain, vbias, w, xs, xr, own, ps, pr, kv, mask,
    local_sem, x_sem, wsem, xsend, xrecv, psend, precv, ssend, srecv, fsend,
):
    tokens, depth = x.shape
    chips = n // 2
    rows = w_hbm.shape[0]
    half = 2 * rows
    mine = lax.axis_index("fsdp")
    i = lax.axis_index("sp")
    core = lax.rem(mine, 2)
    chip = mine // 2
    mate = chip * 2 + (1 - core)
    step = tokens // XCH

    barrier = pltpu.get_barrier_semaphore()
    pl.semaphore_signal(barrier, inc=1, device_id={"fsdp": mate})
    for o in range(1, chips):
        peer = lax.rem(chip + o, chips) * 2 + core
        pl.semaphore_signal(barrier, inc=1, device_id={"fsdp": peer})
    for b in range(1, reach + 1):
        @pl.when(i >= b)
        def _():
            pl.semaphore_signal(barrier, inc=1, device_id={"sp": i - b})

        @pl.when(i + b < s)
        def _():
            pl.semaphore_signal(barrier, inc=1, device_id={"sp": i + b})

    def xcopy(c):
        part = pl.ds(c * step, step)
        return pltpu.make_async_copy(x_hbm.at[part], x.at[part], x_sem.at[c])

    gcopy = pltpu.make_async_copy(gain_hbm, gain, local_sem.at[0])
    gcopy.start()
    dcopy = pltpu.make_async_copy(docs_hbm, docs, local_sem.at[4])
    dcopy.start()
    for c in range(XCH):
        xcopy(c).start()
    wcopy = pltpu.make_async_copy(w_hbm, w.at[core], local_sem.at[1])
    qcopy = pltpu.make_async_copy(q_hbm, q, local_sem.at[2])
    bcopy = pltpu.make_async_copy(vbias_hbm, vbias, local_sem.at[3])

    def wsend():
        return pltpu.make_async_remote_copy(
            w_hbm, w.at[core], wsem.at[0], wsem.at[1], device_id={"fsdp": mate}
        )

    def xsendcopy(o, c):
        target = lax.rem(chip + o, chips)
        part = pl.ds(c * step, step)
        return pltpu.make_async_remote_copy(
            xs.at[target, part], xr.at[o - 1, part], xsend.at[o - 1, c], xrecv.at[o - 1, c],
            device_id={"fsdp": target * 2 + core},
        )

    gcopy.wait()
    dcopy.wait()
    for c in range(XCH):
        xcopy(c).wait()
        part = slice(c * step, (c + 1) * step)
        wide = x[part, :].astype(jnp.float32)
        inv = lax.rsqrt(jnp.mean(wide * wide, axis=-1, keepdims=True) + EPS)
        for t in range(chips):
            piece = x[part, t * half:(t + 1) * half].astype(jnp.float32)
            piece = piece * inv * gain[:, t * half:(t + 1) * half]
            xs[t, part, :] = piece.astype(jnp.bfloat16)
        if c == 0:
            near = jnp.minimum(i, reach) + jnp.minimum(s - 1 - i, reach)
            pl.semaphore_wait(barrier, chips + near)
        for o in range(1, chips):
            xsendcopy(o, c).start()
        if c == 0:
            wsend().start()
            wcopy.start()
            bcopy.start()
            qcopy.start()

    first = i * tokens
    width = reach * tokens + QB
    for u in range(tokens // QB):
        pos = first + u * QB + lax.broadcasted_iota(jnp.int32, (QB, 1), 0)
        start = jnp.zeros((QB, 1), jnp.int32)
        end = jnp.int32(0)
        for d in range(docs.shape[1]):
            end = end + docs[0, d]
            start = jnp.where(pos >= end, end, start)
        key = first + u * QB - reach * tokens + lax.broadcasted_iota(jnp.int32, (QB, width), 1)
        mask[u] = jnp.where((key >= start) & (key <= pos), 0.0, MASKED)
    for b in range(1, reach + 1):
        @pl.when(i < b)
        def _():
            kv[:, (reach - b) * tokens:(reach - b + 1) * tokens, :] = jnp.zeros(
                (MSGS, tokens, HD), jnp.bfloat16
            )

    def project(left, j, kind):
        cols = pl.ds(pl.multiple_of(kind * (KVH * HD) + j * PAIR, PAIR), PAIR)
        total = jnp.dot(left[:, :rows], w[0, :, cols], preferred_element_type=jnp.float32)
        return total + jnp.dot(
            left[:, rows:], w[1, :, cols], preferred_element_type=jnp.float32
        )

    wcopy.wait()
    wsend().wait()
    bcopy.wait()
    qcopy.wait()

    @pl.loop(0, PAIRS)
    def _(j):
        keys = project(xs.at[chip], j, 0)
        values = project(xs.at[chip], j, 1)
        values = values + vbias[:, pl.ds(pl.multiple_of(j * PAIR, PAIR), PAIR)]
        for h in range(2):
            own[4 * j + 2 * h] = keys[:, h * HD:(h + 1) * HD]
            own[4 * j + 2 * h + 1] = values[:, h * HD:(h + 1) * HD]

    def psendcopy(o, m, part, k):
        source = lax.rem(chip + chips - o, chips)
        return pltpu.make_async_remote_copy(
            ps.at[o - 1, m, part], pr.at[o - 1, m, part], psend.at[o - 1, k], precv.at[o - 1, k],
            device_id={"fsdp": source * 2 + core},
        )

    whole = pl.ds(0, tokens)
    half_tokens = tokens // 2
    pieces = (pl.ds(0, half_tokens), pl.ds(half_tokens, half_tokens))

    def give_back(o, j, part):
        for kind in range(2):
            partial = project(xr.at[o - 1, part], j, kind).astype(jnp.bfloat16)
            for h in range(2):
                ps[o - 1, 4 * j + 2 * h + kind, part, :] = partial[:, h * HD:(h + 1) * HD]
        for m in range(4):
            if isinstance(j, int) and j == PAIRS - 1 and m >= 2:
                for piece in range(2):
                    psendcopy(o, 4 * j + m, pieces[piece], 4 * j + m + 2 * piece).start()
            else:
                psendcopy(o, 4 * j + m, part, 4 * j + m).start()

    ahead = XCH - 2
    early = pl.ds(0, ahead * step)
    late = pl.ds(ahead * step, tokens - ahead * step)
    for o in range(1, chips):
        for c in range(ahead):
            xsendcopy(o, c).wait_recv()
        give_back(o, 0, early)
    for o in range(1, chips):
        for c in range(ahead, XCH):
            xsendcopy(o, c).wait_recv()
        give_back(o, 0, late)

    @pl.loop(1, PAIRS - 1)
    def _(j):
        for o in range(1, chips):
            give_back(o, j, whole)

    for o in range(1, chips):
        give_back(o, PAIRS - 1, whole)

    def rows_of(piece):
        return whole if piece is None else pieces[piece]

    def seat(m, piece):
        return m if piece is None else m + 2 * piece

    def slot(b, piece=None):
        base = (reach - b) * tokens
        if piece is None:
            return pl.ds(base, tokens)
        return pl.ds(base + piece * half_tokens, half_tokens)

    def shiftcopy(b, m, piece=None):
        k = seat(m, piece)
        return pltpu.make_async_remote_copy(
            kv.at[m, slot(0, piece)], kv.at[m, slot(b, piece)], ssend.at[b - 1, k],
            srecv.at[b - 1, k], device_id={"sp": i + b},
        )

    def relay(m, piece=None):
        k = seat(m, piece)
        return pltpu.make_async_remote_copy(
            kv.at[m, slot(2, piece)], kv.at[m, slot(1, piece)], fsend.at[k], srecv.at[0, k],
            device_id={"sp": i - 1},
        )

    odd = lax.rem(i, 2) == 1

    def sends(b):
        return (i + b < s) & jnp.logical_not(odd) if b == 1 else i + b < s

    def finish(m, piece=None):
        rows_m = rows_of(piece)
        total = own[m, rows_m]
        for o in range(1, chips):
            psendcopy(o, m, rows_m, seat(m, piece)).wait_recv()
            total = total + pr[o - 1, m, rows_m].astype(jnp.float32)
        kv[m, slot(0, piece), :] = total.astype(jnp.bfloat16)
        for b in range(reach, 0, -1):
            @pl.when(sends(b))
            def _():
                shiftcopy(b, m, piece).start()

    def pass_on(m, piece=None):
        @pl.when(i >= 2)
        def _():
            shiftcopy(2, m, piece).wait_recv()

        @pl.when(odd & (i >= 3))
        def _():
            relay(m, piece).start()

    def arrive(m, piece=None):
        for b in range(1, reach + 1):
            if b != 2:
                @pl.when(i >= b)
                def _():
                    shiftcopy(b, m, piece).wait_recv()

    factor = HD ** (-0.5) * math.log2(math.e)
    ratio = QH // KVH

    def attend(g, u):
        base = g * ratio * HD
        if not isinstance(g, int):
            base = pl.multiple_of(base, HD)
        left = jnp.concatenate(
            [q[u * QB:(u + 1) * QB, pl.ds(base + r * HD, HD)] for r in range(ratio)], 0
        )
        keys = kv[2 * g, u * QB:u * QB + width, :]
        values = kv[2 * g + 1, u * QB:u * QB + width, :]
        scores = lax.dot_general(
            left, keys, (((1,), (1,)), ((), ())), preferred_element_type=jnp.float32
        )
        scores = scores.reshape(ratio, QB, width) + mask[u][None]
        scores = scores.reshape(ratio * QB, width)
        highest = jnp.max(scores, axis=-1, keepdims=True)
        probs = jnp.exp2((scores - highest) * factor)
        total = jnp.sum(probs, axis=-1, keepdims=True)
        result = jnp.dot(
            probs.astype(jnp.bfloat16), values, preferred_element_type=jnp.float32
        )
        result = (result / total).astype(jnp.bfloat16)
        for r in range(ratio):
            out[u * QB:(u + 1) * QB, pl.ds(base + r * HD, HD)] = result[
                r * QB:(r + 1) * QB
            ]

    def when(condition, action):
        @pl.when(condition)
        def _():
            action()

    def opening(g):
        arrive(2 * g)
        arrive(2 * g + 1)
        attend(g, 0)

    @pl.loop(0, KVH - 1)
    def _(t):
        finish(2 * t)
        when(t >= 2, lambda: pass_on(2 * t - 3))
        when(t >= 4, lambda: attend(t - 4, 1))
        finish(2 * t + 1)
        when(t >= 1, lambda: pass_on(2 * t - 2))
        when(t >= 3, lambda: opening(t - 3))

    finish(LAST, 0)
    pass_on(LAST - 3)
    attend(KVH - 5, 1)
    finish(LAST, 1)
    finish(LAST + 1, 0)
    pass_on(LAST - 2)
    opening(KVH - 4)
    finish(LAST + 1, 1)
    pass_on(LAST - 1)
    pass_on(LAST, 0)
    attend(KVH - 4, 1)
    pass_on(LAST, 1)
    opening(KVH - 3)
    pass_on(LAST + 1, 0)
    pass_on(LAST + 1, 1)
    attend(KVH - 3, 1)
    opening(KVH - 2)
    attend(KVH - 2, 1)
    for piece in range(2):
        arrive(LAST, piece)
        arrive(LAST + 1, piece)
    attend(KVH - 1, 0)
    attend(KVH - 1, 1)

    for o in range(1, chips):
        for c in range(XCH):
            xsendcopy(o, c).wait_send()

    def settle(m, piece=None):
        for o in range(1, chips):
            psendcopy(o, m, rows_of(piece), seat(m, piece)).wait_send()
        for b in range(1, reach + 1):
            when(sends(b), lambda: shiftcopy(b, m, piece).wait_send())
        when(odd & (i >= 3), lambda: relay(m, piece).wait_send())

    @pl.loop(0, LAST)
    def _(m):
        settle(m)

    for piece in range(2):
        settle(LAST, piece)
        settle(LAST + 1, piece)


def shards(n, s, hidden, queries, norm_gain, kv_weight, value_bias, doc_lengths):
    _, tokens, depth = hidden.shape
    reach = s // 4
    chips = n // 2
    rows = kv_weight.shape[0]
    far = chips - 1
    vmem = pltpu.VMEM
    dma = pltpu.SemaphoreType.DMA
    hold = lambda a: pltpu.with_memory_space_constraint(a, pltpu.HBM)
    anywhere = pl.BlockSpec(memory_space=pltpu.HBM)
    result = pl.pallas_call(
        functools.partial(kernel, n, s, reach),
        out_shape=jax.ShapeDtypeStruct((tokens, QH * HD), jnp.bfloat16),
        in_specs=[anywhere] * 6,
        out_specs=pl.BlockSpec(memory_space=pltpu.VMEM),
        scratch_shapes=[
            pltpu.SMEM((1, doc_lengths.shape[1]), jnp.int32),
            vmem((tokens, depth), jnp.bfloat16),
            vmem((tokens, QH * HD), jnp.bfloat16),
            vmem((1, depth), jnp.float32),
            vmem((1, KVH * HD), jnp.float32),
            vmem((2, rows, 2 * KVH * HD), jnp.bfloat16),
            vmem((chips, tokens, 2 * rows), jnp.bfloat16),
            vmem((far, tokens, 2 * rows), jnp.bfloat16),
            vmem((MSGS, tokens, HD), jnp.float32),
            vmem((far, MSGS, tokens, HD), jnp.bfloat16),
            vmem((far, MSGS, tokens, HD), jnp.bfloat16),
            vmem((MSGS, (reach + 1) * tokens, HD), jnp.bfloat16),
            vmem((tokens // QB, QB, reach * tokens + QB), jnp.float32),
            dma((5,)),
            dma((XCH,)),
            dma((2,)),
            dma((far, XCH)),
            dma((far, XCH)),
            dma((far, SEATS)),
            dma((far, SEATS)),
            dma((reach, SEATS)),
            dma((reach, SEATS)),
            dma((SEATS,)),
        ],
        compiler_params=pltpu.CompilerParams(
            collective_id=0, has_side_effects=True, vmem_limit_bytes=50 * 1024 * 1024
        ),
    )(
        hidden[0], queries[0], hold(norm_gain.reshape(1, depth)), kv_weight,
        hold(value_bias.reshape(1, KVH * HD)), hold(doc_lengths),
    )
    return result.reshape(1, tokens, QH * HD)


def solution(mesh):
    in_specs = (
        P("fsdp", "sp", None),
        P("fsdp", "sp", None),
        P(),
        P("fsdp", None),
        P(),
        P("fsdp", None),
    )
    body = functools.partial(shards, mesh.shape["fsdp"], mesh.shape["sp"])
    return jax.shard_map(
        body, mesh=mesh, in_specs=in_specs, out_specs=P("fsdp", "sp", None), check_vma=False
    )
```

```python
import functools
import math

import jax
import jax.numpy as jnp
from jax import lax
from jax.experimental import pallas as pl
from jax.experimental.pallas import tpu as pltpu
from jax.sharding import PartitionSpec as P

QH = 32
KVH = 8
HD = 128
EPS = 1e-06
PAIR = 2 * HD
PAIRS = KVH // 2
MSGS = 2 * KVH
LAST = MSGS - 2
SPLIT = 4
SEATS = MSGS + 2 + SPLIT
FIRST, SECOND, EARLY, LATE = range(4)
XCH = 8
QB = 128
MASKED = -1e30
SHARE = 3
PARTS = 2


def aligned(index, step):
    return index if isinstance(index, int) else pl.multiple_of(index, step)


def kernel(
    n, s, reach, give,
    x_hbm, q_hbm, gain_hbm, w_hbm, vbias_hbm, docs_hbm,
    out,
    docs, x, q, res, gain, vbias, w, xs, xr, own, ps, pr, kv, mask,
    local_sem, x_sem, wsem, xsend, xrecv, psend, precv, ssend, srecv, fsend, osem,
    *gather,
):
    tokens, depth = x.shape
    chips = n // 2
    rows = w_hbm.shape[0]
    half = 2 * rows
    kept = rows - give
    sent = 2 * kept
    mine = lax.axis_index("fsdp")
    i = lax.axis_index("sp")
    core = lax.rem(mine, 2)
    chip = mine // 2
    mate = chip * 2 + (1 - core)
    step = tokens // XCH

    barrier = pltpu.get_barrier_semaphore()
    pl.semaphore_signal(barrier, inc=1, device_id={"fsdp": mate})
    for o in range(1, chips):
        peer = lax.rem(chip + o, chips) * 2 + core
        pl.semaphore_signal(barrier, inc=1, device_id={"fsdp": peer})
    if give:
        for o in range(1, s):
            pl.semaphore_signal(barrier, inc=1, device_id={"sp": lax.rem(i + o, s)})
        callers = chips + s - 1
    else:
        for b in range(1, reach + 1):
            @pl.when(i >= b)
            def _():
                pl.semaphore_signal(barrier, inc=1, device_id={"sp": i - b})

            @pl.when(i + b < s)
            def _():
                pl.semaphore_signal(barrier, inc=1, device_id={"sp": i + b})
        callers = chips + jnp.minimum(i, reach) + jnp.minimum(s - 1 - i, reach)

    def take(sem, ref):
        pltpu.make_async_copy(ref, ref, sem).wait()

    def xcopy(c):
        part = pl.ds(c * step, step)
        return pltpu.make_async_copy(x_hbm.at[part], x.at[part], x_sem.at[c])

    gcopy = pltpu.make_async_copy(gain_hbm, gain.at[:, pl.ds(0, depth)], local_sem.at[0])
    gcopy.start()
    dcopy = pltpu.make_async_copy(docs_hbm, docs, local_sem.at[4])
    dcopy.start()
    for c in range(XCH):
        xcopy(c).start()
    qcopy = pltpu.make_async_copy(q_hbm, q, local_sem.at[2])
    bcopy = pltpu.make_async_copy(vbias_hbm, vbias, local_sem.at[3])

    bands = [(pl.ds(give, kept), pl.ds(core * kept, kept))]
    if give:
        bands.append((pl.ds(0, give), pl.ds(sent + core * give, give)))

    def wcopies():
        return [
            pltpu.make_async_copy(w_hbm.at[a], w.at[b], local_sem.at[(1, 5)[k]])
            for k, (a, b) in enumerate(bands)
        ]

    def wsends():
        return [
            pltpu.make_async_remote_copy(
                w_hbm.at[a], w.at[b], wsem.at[k, 0], wsem.at[k, 1], device_id={"fsdp": mate}
            )
            for k, (a, b) in enumerate(bands)
        ]

    def xsendcopy(o, c):
        target = lax.rem(chip + o, chips)
        part = pl.ds(c * step, step)
        return pltpu.make_async_remote_copy(
            xs.at[target, part, pl.ds(0, sent)], xr.at[o - 1, part], xsend.at[o - 1],
            xrecv.at[o - 1, c // (XCH - 2)], device_id={"fsdp": target * 2 + core},
        )

    if give:
        wg, ysend, yrecv, zsend, hsend, grecv, msend, mrecv = gather
        parts, _, wide_cols = wg.shape
        strip = give // s
        lines = s // 2
        beside = i + 1 - 2 * lax.rem(i, 2)

        def slab(c, k):
            return pl.ds(pl.multiple_of(c * give + k * strip, 16), strip)

        def ygive(h, kind):
            span = wide_cols // 2
            return pltpu.make_async_remote_copy(
                w_hbm.at[pl.ds(pl.multiple_of(i * strip, 16), strip),
                         pl.ds(kind * (KVH * HD) + h * span, span)],
                wg.at[h, slab(core, i), pl.ds(kind * span, span)],
                ysend.at[h], yrecv.at[h],
                device_id={"fsdp": (1 - chip) * 2 + core},
            )

        def zgive(h, k, up):
            return pltpu.make_async_remote_copy(
                wg.at[h, slab(core, k)], wg.at[h, slab(core, k)], zsend.at[h, up],
                grecv.at[h, k], device_id={"sp": i + (2 if up else -2)},
            )

        def has(up):
            return i + 2 < s if up else i >= 2

        def hgive(h, k):
            return pltpu.make_async_remote_copy(
                wg.at[h, slab(core, k)], wg.at[h, slab(core, k)], hsend.at[h],
                grecv.at[h, k], device_id={"sp": beside},
            )

        def mgive(h, k, c):
            return pltpu.make_async_remote_copy(
                wg.at[h, slab(c, k)], wg.at[h, slab(c, k)], msend.at[h], mrecv.at[h],
                device_id={"fsdp": mate},
            )

        def spread(h):
            take(yrecv.at[h], wg.at[h, slab(core, i)])
            for up in (1, 0):
                @pl.when(has(up))
                def _():
                    zgive(h, i, up).start()
            hgive(h, i).start()
            mgive(h, i, core).start()

        def across(h, d):
            for up in (1, 0):
                k = i - 2 * d if up else i + 2 * d

                @pl.when(k >= 0 if up else k < s)
                def _():
                    hgive(h, k).wait_recv()

                    @pl.when(has(up))
                    def _():
                        zgive(h, k, up).start()

                    hgive(h, k).start()
                    mgive(h, k, core).start()

        def inward(h, o):
            k = lax.rem(beside + s - 2 * o, s)
            hgive(h, k).wait_recv()
            mgive(h, k, core).start()

        def gathered(h):
            take(mrecv.at[h], wg.at[h, pl.ds(pl.multiple_of((1 - core) * give, 16), give)])

        def regain():
            for h in range(parts):
                take(ysend.at[h], wg.at[h, pl.ds(0, strip)])
                take(hsend.at[h], wg.at[h, pl.ds(0, lines * strip)])
                take(msend.at[h], wg.at[h, pl.ds(0, give)])
                for up in (1, 0):
                    for d in range(lines - 1):
                        passed = i // 2 if up else lines - 1 - i // 2

                        @pl.when(passed == d)
                        def _():
                            take(zsend.at[h, up], wg.at[h, pl.ds(0, (d + 1) * strip)])

    pieces_of = [(0, give, kept), (kept, rows + give, kept)]
    if give:
        pieces_of += [(sent, 0, give), (sent + give, rows, give)]
    gcopy.wait()
    dcopy.wait()
    for c in range(XCH):
        xcopy(c).wait()
        part = slice(c * step, (c + 1) * step)
        wide = x[part, :].astype(jnp.float32)
        inv = lax.rsqrt(jnp.mean(wide * wide, axis=-1, keepdims=True) + EPS)
        for t in range(chips):
            for to, at, size in pieces_of:
                cut = slice(t * half + at, t * half + at + size)
                piece = x[part, cut].astype(jnp.float32) * inv * gain[:, cut]
                xs[t, part, to:to + size] = piece.astype(jnp.bfloat16)
        if c == 0:
            pl.semaphore_wait(barrier, callers)
            if give:
                for h in range(parts):
                    for kind in range(2):
                        ygive(h, kind).start()
        for o in range(1, chips):
            xsendcopy(o, c).start()
        if c == 0:
            for copy in wsends() + wcopies():
                copy.start()
            bcopy.start()
            qcopy.start()

    first = i * tokens
    width = reach * tokens + QB
    for u in range(tokens // QB):
        pos = first + u * QB + lax.broadcasted_iota(jnp.int32, (QB, 1), 0)
        start = jnp.zeros((QB, 1), jnp.int32)
        end = jnp.int32(0)
        for d in range(docs.shape[1]):
            end = end + docs[0, d]
            start = jnp.where(pos >= end, end, start)
        key = first + u * QB - reach * tokens + lax.broadcasted_iota(jnp.int32, (QB, width), 1)
        mask[u] = jnp.where((key >= start) & (key <= pos), 0.0, MASKED)
    for b in range(1, reach + 1):
        @pl.when(i < b)
        def _():
            kv[:, (reach - b) * tokens:(reach - b + 1) * tokens, :] = jnp.zeros(
                (MSGS, tokens, HD), jnp.bfloat16
            )

    def project(left, right, j, kind):
        cols = pl.ds(aligned(kind * (KVH * HD) + j * PAIR, PAIR), PAIR)
        return jnp.dot(left[...], right[:, cols], preferred_element_type=jnp.float32)

    if give:
        for h in range(parts):
            spread(h)
        across(0, 1)
    for copy in wcopies():
        copy.wait()
    for copy in wsends():
        copy.wait()
    bcopy.wait()
    qcopy.wait()

    def own_pair(j):
        keys = project(xs.at[chip], w, j, 0)
        values = project(xs.at[chip], w, j, 1)
        values = values + vbias[:, pl.ds(aligned(j * PAIR, PAIR), PAIR)]
        for h in range(2):
            own[4 * j + 2 * h] = keys[:, h * HD:(h + 1) * HD]
            own[4 * j + 2 * h + 1] = values[:, h * HD:(h + 1) * HD]

    def own_rest(j):
        left = xs[1 - chip, :, sent:]
        group = PAIRS // parts
        h = j // group
        for kind in range(2):
            cols = pl.ds((kind * group + j % group) * PAIR, PAIR)
            more = jnp.dot(left, wg[h, :, cols], preferred_element_type=jnp.float32)
            for r in range(2):
                own[4 * j + 2 * r + kind] += more[:, r * HD:(r + 1) * HD]

    if give:
        turns = [(h, d) for d in range(1, lines) for h in range(parts)][1:]
        for j in range(PAIRS):
            own_pair(j)
            for turn in turns[j:j + 1]:
                across(*turn)
        for turn in turns[PAIRS:]:
            across(*turn)
        for o in range(lines):
            inward(0, o)
    else:
        @pl.loop(0, PAIRS)
        def _(j):
            own_pair(j)

    half_tokens = tokens // 2
    ahead = (XCH - 2) * step
    spans = {
        None: (0, tokens),
        FIRST: (0, half_tokens),
        SECOND: (half_tokens, half_tokens),
        EARLY: (0, ahead),
        LATE: (ahead, tokens - ahead),
    }

    def rows_of(piece):
        return pl.ds(*spans[piece])

    def seat(m, piece):
        return m + {SECOND: 2, LATE: MSGS + 2}.get(piece, 0)

    def psendcopy(o, m, piece):
        source = lax.rem(chip + chips - o, chips)
        k = seat(m, piece)
        return pltpu.make_async_remote_copy(
            ps.at[o - 1, m, rows_of(piece)], pr.at[o - 1, m, rows_of(piece)],
            psend.at[o - 1], precv.at[o - 1, k], device_id={"fsdp": source * 2 + core},
        )

    def give_back(o, j, piece):
        part = rows_of(piece)
        for kind in range(2):
            partial = project(
                xr.at[o - 1, part], w.at[pl.ds(0, sent)], j, kind
            ).astype(jnp.bfloat16)
            for h in range(2):
                ps[o - 1, 4 * j + 2 * h + kind, part, :] = partial[:, h * HD:(h + 1) * HD]
        for m in range(4 * j, 4 * j + 4):
            for cut in (FIRST, SECOND) if m >= LAST else (piece,):
                psendcopy(o, m, cut).start()

    def slot(b, piece):
        start, size = spans[piece]
        return pl.ds((reach - b) * tokens + start, size)

    def shiftcopy(b, m, piece):
        k = seat(m, piece)
        return pltpu.make_async_remote_copy(
            kv.at[m, slot(0, piece)], kv.at[m, slot(b, piece)], ssend.at[b - 1],
            srecv.at[b - 1, k], device_id={"sp": i + b},
        )

    def relay(m, piece):
        k = seat(m, piece)
        return pltpu.make_async_remote_copy(
            kv.at[m, slot(2, piece)], kv.at[m, slot(1, piece)], fsend.at[0], srecv.at[0, k],
            device_id={"sp": i - 1},
        )

    odd = lax.rem(i, 2) == 1

    def sends(b):
        return (i + b < s) & jnp.logical_not(odd) if b == 1 else i + b < s

    def finish(m, piece):
        part = rows_of(piece)
        total = own[m, part]
        for o in range(1, chips):
            psendcopy(o, m, piece).wait_recv()
            total = total + pr[o - 1, m, part].astype(jnp.float32)
        kv[m, slot(0, piece), :] = total.astype(jnp.bfloat16)
        for b in range(reach, 0, -1):
            @pl.when(sends(b))
            def _():
                shiftcopy(b, m, piece).start()

    def pass_on(m, piece):
        @pl.when(i >= 2)
        def _():
            shiftcopy(2, m, piece).wait_recv()

        @pl.when(odd & (i >= 3))
        def _():
            relay(m, piece).start()

    def arrive(m, piece):
        for b in range(1, reach + 1):
            if b != 2:
                @pl.when(i >= b)
                def _():
                    shiftcopy(b, m, piece).wait_recv()

    factor = HD ** (-0.5) * math.log2(math.e)
    ratio = QH // KVH

    def outcopy(g, u):
        block = (
            pl.ds(u * QB, QB), pl.ds(aligned(g * ratio * HD, ratio * HD), ratio * HD)
        )
        return pltpu.make_async_copy(res.at[block], out.at[block], osem.at[0])

    def attend(g, u):
        base = aligned(g * ratio * HD, HD)
        left = jnp.concatenate(
            [q[u * QB:(u + 1) * QB, pl.ds(base + r * HD, HD)] for r in range(ratio)], 0
        )
        keys = kv[2 * g, u * QB:u * QB + width, :]
        values = kv[2 * g + 1, u * QB:u * QB + width, :]
        scores = lax.dot_general(
            left, keys, (((1,), (1,)), ((), ())), preferred_element_type=jnp.float32
        )
        scores = scores.reshape(ratio, QB, width) + mask[u][None]
        scores = scores.reshape(ratio * QB, width)
        highest = jnp.max(scores, axis=-1, keepdims=True)
        probs = jnp.exp2((scores - highest) * factor)
        total = jnp.sum(probs, axis=-1, keepdims=True)
        result = jnp.dot(
            probs.astype(jnp.bfloat16), values, preferred_element_type=jnp.float32
        )
        result = (result / total).astype(jnp.bfloat16)
        for r in range(ratio):
            res[u * QB:(u + 1) * QB, pl.ds(base + r * HD, HD)] = result[
                r * QB:(r + 1) * QB
            ]
        outcopy(g, u).start()

    def when(condition, action):
        @pl.when(condition)
        def _():
            action()

    def cuts(m):
        if m < SPLIT:
            return (EARLY, LATE)
        return (FIRST, SECOND) if m >= LAST else (None,)

    def finish_all(messages, piece):
        for m in messages:
            finish(m, piece)

    def pass_all(messages, piece):
        for m in messages:
            pass_on(m, piece)

    def first_rest():
        if give:
            for h in range(1, parts):
                for o in range(lines):
                    inward(h, o)
            gathered(0)
            for j in range(PAIRS // parts):
                own_rest(j)

    def later_rest():
        if give:
            for h in range(1, parts):
                gathered(h)
                for j in range(PAIRS // parts * h, PAIRS // parts * (h + 1)):
                    own_rest(j)

    def give_all(j, piece):
        for o in range(1, chips):
            give_back(o, j, piece)

    for o in range(1, chips):
        take(xrecv.at[o - 1, 0], xr.at[o - 1, rows_of(EARLY)])
        give_back(o, 0, EARLY)
    first_rest()
    for o in range(1, chips):
        take(xrecv.at[o - 1, 1], xr.at[o - 1, rows_of(LATE)])
        give_back(o, 0, LATE)
    for j in range(1, PAIRS):
        give_all(j, None)
        finish(j - 1, EARLY)
    later_rest()
    finish(SPLIT - 1, EARLY)
    finish_all(range(SPLIT), LATE)
    pass_all(range(SPLIT), EARLY)
    finish(SPLIT, None)
    pass_all(range(SPLIT), LATE)
    finish(SPLIT + 1, None)

    due = {}
    for g in range(4):
        for u in range(2):
            due[g, u] = ((2 * g + 6 + u, None),), ((2 * g + 4 + u, None),)
    due[4, 0] = ((LAST, FIRST), (LAST, SECOND)), ((LAST - 2, None),)
    due[4, 1] = ((LAST + 1, FIRST), (LAST + 1, SECOND)), ((LAST - 1, None),)
    due[5, 0] = (), ((LAST, FIRST),)
    due[5, 1] = (), ((LAST, SECOND), (LAST + 1, FIRST))
    due[6, 0] = (), ((LAST + 1, SECOND),)

    def serve(g, u):
        finishing, passing = due[g, u]
        for unit in finishing:
            finish(*unit)
        for unit in passing:
            pass_on(*unit)

    def ready(g):
        for m in (2 * g, 2 * g + 1):
            for cut in cuts(m):
                arrive(m, cut)

    @pl.loop(0, KVH)
    def _(g):
        for u in range(tokens // QB):
            for turn in range(KVH):
                if (turn, u) in due:
                    when(g == turn, functools.partial(serve, turn, u))
                if u == 0:
                    when(g == turn, functools.partial(ready, turn))
            attend(g, u)

    for o in range(1, chips):
        take(xsend.at[o - 1], xr.at[o - 1])
        take(psend.at[o - 1], ps.at[o - 1])
    for b in range(1, reach + 1):
        when(sends(b), functools.partial(take, ssend.at[b - 1], kv.at[:, slot(0, None)]))
    when(odd & (i >= 3), functools.partial(take, fsend.at[0], kv.at[:, slot(2, None)]))
    if give:
        regain()
    pltpu.make_async_copy(res, out, osem.at[0]).wait()


def shards(n, s, hidden, queries, norm_gain, kv_weight, value_bias, doc_lengths):
    _, tokens, depth = hidden.shape
    reach = s // 4
    chips = n // 2
    rows = kv_weight.shape[0]
    far = chips - 1
    give = rows * SHARE // 10 // HD * HD if chips == 2 and s % 2 == 0 else 0
    if give % (16 * s):
        give = 0
    kept = rows - give
    vmem = pltpu.VMEM
    dma = pltpu.SemaphoreType.DMA
    taken = [
        vmem((PARTS, 2 * give, 2 * KVH * HD // PARTS), jnp.bfloat16),
        dma((PARTS,)),
        dma((PARTS,)),
        dma((PARTS, 2)),
        dma((PARTS,)),
        dma((PARTS, s)),
        dma((PARTS,)),
        dma((PARTS,)),
    ] if give else []
    hold = lambda a: pltpu.with_memory_space_constraint(a, pltpu.HBM)
    anywhere = pl.BlockSpec(memory_space=pltpu.HBM)
    result = pl.pallas_call(
        functools.partial(kernel, n, s, reach, give),
        out_shape=jax.ShapeDtypeStruct((tokens, QH * HD), jnp.bfloat16),
        in_specs=[anywhere] * 6,
        out_specs=anywhere,
        scratch_shapes=[
            pltpu.SMEM((1, doc_lengths.shape[1]), jnp.int32),
            vmem((tokens, depth), jnp.bfloat16),
            vmem((tokens, QH * HD), jnp.bfloat16),
            vmem((tokens, QH * HD), jnp.bfloat16),
            vmem((1, depth + 8 * HD), jnp.float32),
            vmem((1, KVH * HD), jnp.float32),
            vmem((2 * rows, 2 * KVH * HD), jnp.bfloat16),
            vmem((chips, tokens, 2 * rows), jnp.bfloat16),
            vmem((far, tokens, 2 * kept), jnp.bfloat16),
            vmem((MSGS, tokens, HD), jnp.float32),
            vmem((far, MSGS, tokens, HD), jnp.bfloat16),
            vmem((far, MSGS, tokens, HD), jnp.bfloat16),
            vmem((MSGS, (reach + 1) * tokens, HD), jnp.bfloat16),
            vmem((tokens // QB, QB, reach * tokens + QB), jnp.float32),
            dma((6,)),
            dma((XCH,)),
            dma((2, 2)),
            dma((far,)),
            dma((far, 2)),
            dma((far,)),
            dma((far, SEATS)),
            dma((reach,)),
            dma((reach, SEATS)),
            dma((1,)),
            dma((1,)),
        ] + taken,
        compiler_params=pltpu.CompilerParams(
            collective_id=0, has_side_effects=True, vmem_limit_bytes=50 * 1024 * 1024
        ),
    )(
        hidden[0], queries[0], hold(norm_gain.reshape(1, depth)), kv_weight,
        hold(value_bias.reshape(1, KVH * HD)), hold(doc_lengths),
    )
    return result.reshape(1, tokens, QH * HD)


def solution(mesh):
    in_specs = (
        P("fsdp", "sp", None),
        P("fsdp", "sp", None),
        P(),
        P("fsdp", None),
        P(),
        P("fsdp", None),
    )
    body = functools.partial(shards, mesh.shape["fsdp"], mesh.shape["sp"])
    return jax.shard_map(
        body, mesh=mesh, in_specs=in_specs, out_specs=P("fsdp", "sp", None), check_vma=False
    )
```

```python
import functools
import math

import jax
import jax.numpy as jnp
from jax import lax
from jax.experimental import pallas as pl
from jax.experimental.pallas import tpu as pltpu
from jax.sharding import PartitionSpec as P

QH = 32
KVH = 8
HD = 128
EPS = 1e-06
PAIR = 2 * HD
PAIRS = KVH // 2
MSGS = 2 * KVH
LAST = MSGS - 2
SPLIT = 4
LEAD = 6
NEAR = 5
SEATS = MSGS + 2 + SPLIT
FIRST, SECOND, EARLY, LATE = range(4)
XCH = 8
QB = 128
MASKED = -1e30
SHARE = 3
PARTS = 2


def aligned(index, step):
    return index if isinstance(index, int) else pl.multiple_of(index, step)


def kernel(
    n, s, reach, give,
    x_hbm, q_hbm, gain_hbm, w_hbm, vbias_hbm, docs_hbm,
    out,
    docs, x, q, res, gain, vbias, w, xs, xr, own, ps, pr, kv, mask,
    local_sem, x_sem, wsem, xsend, xrecv, psend, precv, ssend, srecv, fsend, osem,
    *gather,
):
    tokens, depth = x.shape
    chips = n // 2
    rows = w_hbm.shape[0]
    half = 2 * rows
    kept = rows - give
    sent = 2 * kept
    mine = lax.axis_index("fsdp")
    i = lax.axis_index("sp")
    core = lax.rem(mine, 2)
    chip = mine // 2
    mate = chip * 2 + (1 - core)
    step = tokens // XCH

    barrier = pltpu.get_barrier_semaphore()
    pl.semaphore_signal(barrier, inc=1, device_id={"fsdp": mate})
    for o in range(1, chips):
        peer = lax.rem(chip + o, chips) * 2 + core
        pl.semaphore_signal(barrier, inc=1, device_id={"fsdp": peer})
    if give:
        for o in range(1, s):
            pl.semaphore_signal(barrier, inc=1, device_id={"sp": lax.rem(i + o, s)})
        callers = chips + s - 1
    else:
        for b in range(1, reach + 1):
            @pl.when(i >= b)
            def _():
                pl.semaphore_signal(barrier, inc=1, device_id={"sp": i - b})

            @pl.when(i + b < s)
            def _():
                pl.semaphore_signal(barrier, inc=1, device_id={"sp": i + b})
        callers = chips + jnp.minimum(i, reach) + jnp.minimum(s - 1 - i, reach)

    def take(sem, ref):
        pltpu.make_async_copy(ref, ref, sem).wait()

    def xcopy(c):
        part = pl.ds(c * step, step)
        return pltpu.make_async_copy(x_hbm.at[part], x.at[part], x_sem.at[c])

    gcopy = pltpu.make_async_copy(gain_hbm, gain.at[:, pl.ds(0, depth)], local_sem.at[0])
    gcopy.start()
    dcopy = pltpu.make_async_copy(docs_hbm, docs, local_sem.at[4])
    dcopy.start()
    for c in range(XCH):
        xcopy(c).start()
    qcopy = pltpu.make_async_copy(q_hbm, q, local_sem.at[2])
    bcopy = pltpu.make_async_copy(vbias_hbm, vbias, local_sem.at[3])

    bands = [(pl.ds(give, kept), pl.ds(core * kept, kept))]
    if give:
        bands.append((pl.ds(0, give), pl.ds(sent + core * give, give)))

    def wcopies():
        return [
            pltpu.make_async_copy(w_hbm.at[a], w.at[b], local_sem.at[(1, 5)[k]])
            for k, (a, b) in enumerate(bands)
        ]

    def wsends():
        return [
            pltpu.make_async_remote_copy(
                w_hbm.at[a], w.at[b], wsem.at[k, 0], wsem.at[k, 1], device_id={"fsdp": mate}
            )
            for k, (a, b) in enumerate(bands)
        ]

    def xsendcopy(o, c):
        target = lax.rem(chip + o, chips)
        part = pl.ds(c * step, step)
        return pltpu.make_async_remote_copy(
            xs.at[target, part, pl.ds(0, sent)], xr.at[o - 1, part], xsend.at[o - 1],
            xrecv.at[o - 1, c // (XCH - 2)], device_id={"fsdp": target * 2 + core},
        )

    if give:
        wg, ysend, yrecv, zsend, hsend, grecv, msend, mrecv = gather
        parts, _, wide_cols = wg.shape
        strip = give // s
        lines = s // 2
        beside = i + 1 - 2 * lax.rem(i, 2)

        def slab(c, k):
            return pl.ds(pl.multiple_of(c * give + k * strip, 16), strip)

        def ygive(h, kind):
            span = wide_cols // 2
            return pltpu.make_async_remote_copy(
                w_hbm.at[pl.ds(pl.multiple_of(i * strip, 16), strip),
                         pl.ds(kind * (KVH * HD) + h * span, span)],
                wg.at[h, slab(core, i), pl.ds(kind * span, span)],
                ysend.at[h], yrecv.at[h],
                device_id={"fsdp": (1 - chip) * 2 + core},
            )

        def zgive(h, k, up):
            return pltpu.make_async_remote_copy(
                wg.at[h, slab(core, k)], wg.at[h, slab(core, k)], zsend.at[h, up],
                grecv.at[h, k], device_id={"sp": i + (2 if up else -2)},
            )

        def has(up):
            return i + 2 < s if up else i >= 2

        def hgive(h, k):
            return pltpu.make_async_remote_copy(
                wg.at[h, slab(core, k)], wg.at[h, slab(core, k)], hsend.at[h],
                grecv.at[h, k], device_id={"sp": beside},
            )

        def mgive(h, k, c):
            return pltpu.make_async_remote_copy(
                wg.at[h, slab(c, k)], wg.at[h, slab(c, k)], msend.at[h], mrecv.at[h],
                device_id={"fsdp": mate},
            )

        def spread(h):
            take(yrecv.at[h], wg.at[h, slab(core, i)])
            for up in (1, 0):
                @pl.when(has(up))
                def _():
                    zgive(h, i, up).start()
            hgive(h, i).start()
            mgive(h, i, core).start()

        def across(h, d):
            for up in (1, 0):
                k = i - 2 * d if up else i + 2 * d

                @pl.when(k >= 0 if up else k < s)
                def _():
                    hgive(h, k).wait_recv()

                    @pl.when(has(up))
                    def _():
                        zgive(h, k, up).start()

                    hgive(h, k).start()
                    mgive(h, k, core).start()

        def inward(h, o):
            k = lax.rem(beside + s - 2 * o, s)
            hgive(h, k).wait_recv()
            mgive(h, k, core).start()

        def gathered(h):
            take(mrecv.at[h], wg.at[h, pl.ds(pl.multiple_of((1 - core) * give, 16), give)])

        def regain():
            for h in range(parts):
                take(ysend.at[h], wg.at[h, pl.ds(0, strip)])
                take(hsend.at[h], wg.at[h, pl.ds(0, lines * strip)])
                take(msend.at[h], wg.at[h, pl.ds(0, give)])
                for up in (1, 0):
                    for d in range(lines - 1):
                        passed = i // 2 if up else lines - 1 - i // 2

                        @pl.when(passed == d)
                        def _():
                            take(zsend.at[h, up], wg.at[h, pl.ds(0, (d + 1) * strip)])

    pieces_of = [(0, give, kept), (kept, rows + give, kept)]
    if give:
        pieces_of += [(sent, 0, give), (sent + give, rows, give)]
    gcopy.wait()
    dcopy.wait()
    for c in range(XCH):
        xcopy(c).wait()
        part = slice(c * step, (c + 1) * step)
        wide = x[part, :].astype(jnp.float32)
        inv = lax.rsqrt(jnp.mean(wide * wide, axis=-1, keepdims=True) + EPS)
        for t in range(chips):
            for to, at, size in pieces_of:
                cut = slice(t * half + at, t * half + at + size)
                piece = x[part, cut].astype(jnp.float32) * inv * gain[:, cut]
                xs[t, part, to:to + size] = piece.astype(jnp.bfloat16)
        if c == 0:
            pl.semaphore_wait(barrier, callers)
            if give:
                for h in range(parts):
                    for kind in range(2):
                        ygive(h, kind).start()
        for o in range(1, chips):
            xsendcopy(o, c).start()
        if c == 0:
            for copy in wsends() + wcopies():
                copy.start()
            bcopy.start()
            qcopy.start()

    first = i * tokens
    width = reach * tokens + QB
    for u in range(tokens // QB):
        pos = first + u * QB + lax.broadcasted_iota(jnp.int32, (QB, 1), 0)
        start = jnp.zeros((QB, 1), jnp.int32)
        end = jnp.int32(0)
        for d in range(docs.shape[1]):
            end = end + docs[0, d]
            start = jnp.where(pos >= end, end, start)
        key = first + u * QB - reach * tokens + lax.broadcasted_iota(jnp.int32, (QB, width), 1)
        mask[u] = jnp.where((key >= start) & (key <= pos), 0.0, MASKED)
    for b in range(1, reach + 1):
        @pl.when(i < b)
        def _():
            kv[:, (reach - b) * tokens:(reach - b + 1) * tokens, :] = jnp.zeros(
                (MSGS, tokens, HD), jnp.bfloat16
            )

    def project(left, right, j, kind):
        cols = pl.ds(aligned(kind * (KVH * HD) + j * PAIR, PAIR), PAIR)
        return jnp.dot(left[...], right[:, cols], preferred_element_type=jnp.float32)

    if give:
        for h in range(parts):
            spread(h)
        across(0, 1)
    for copy in wcopies():
        copy.wait()
    for copy in wsends():
        copy.wait()
    bcopy.wait()
    qcopy.wait()

    def own_pair(j):
        keys = project(xs.at[chip], w, j, 0)
        values = project(xs.at[chip], w, j, 1)
        values = values + vbias[:, pl.ds(aligned(j * PAIR, PAIR), PAIR)]
        for h in range(2):
            own[4 * j + 2 * h] = keys[:, h * HD:(h + 1) * HD]
            own[4 * j + 2 * h + 1] = values[:, h * HD:(h + 1) * HD]

    def own_rest(j):
        left = xs[1 - chip, :, sent:]
        group = PAIRS // parts
        h = j // group
        for kind in range(2):
            cols = pl.ds((kind * group + j % group) * PAIR, PAIR)
            more = jnp.dot(left, wg[h, :, cols], preferred_element_type=jnp.float32)
            for r in range(2):
                own[4 * j + 2 * r + kind] += more[:, r * HD:(r + 1) * HD]

    if give:
        turns = [(h, d) for d in range(1, lines) for h in range(parts)][1:]
        for j in range(PAIRS):
            own_pair(j)
            for turn in turns[j:j + 1]:
                across(*turn)
        for turn in turns[PAIRS:]:
            across(*turn)
        for o in range(lines):
            inward(0, o)
    else:
        @pl.loop(0, PAIRS)
        def _(j):
            own_pair(j)

    half_tokens = tokens // 2
    ahead = (XCH - 2) * step
    spans = {
        None: (0, tokens),
        FIRST: (0, half_tokens),
        SECOND: (half_tokens, half_tokens),
        EARLY: (0, ahead),
        LATE: (ahead, tokens - ahead),
    }

    def rows_of(piece):
        return pl.ds(*spans[piece])

    def seat(m, piece):
        return m + {SECOND: 2, LATE: MSGS + 2}.get(piece, 0)

    def psendcopy(o, m, piece):
        source = lax.rem(chip + chips - o, chips)
        k = seat(m, piece)
        return pltpu.make_async_remote_copy(
            ps.at[o - 1, m, rows_of(piece)], pr.at[o - 1, m, rows_of(piece)],
            psend.at[o - 1], precv.at[o - 1, k], device_id={"fsdp": source * 2 + core},
        )

    def give_back(o, j, piece):
        part = rows_of(piece)
        for kind in range(2):
            partial = project(
                xr.at[o - 1, part], w.at[pl.ds(0, sent)], j, kind
            ).astype(jnp.bfloat16)
            for h in range(2):
                ps[o - 1, 4 * j + 2 * h + kind, part, :] = partial[:, h * HD:(h + 1) * HD]
        for m in range(4 * j, 4 * j + 4):
            for cut in (FIRST, SECOND) if m >= LAST else (piece,):
                psendcopy(o, m, cut).start()

    def slot(b, piece):
        start, size = spans[piece]
        return pl.ds((reach - b) * tokens + start, size)

    def shiftcopy(b, m, piece):
        k = seat(m, piece)
        return pltpu.make_async_remote_copy(
            kv.at[m, slot(0, piece)], kv.at[m, slot(b, piece)], ssend.at[b - 1],
            srecv.at[b - 1, k], device_id={"sp": i + b},
        )

    def relay(m, piece):
        k = seat(m, piece)
        return pltpu.make_async_remote_copy(
            kv.at[m, slot(2, piece)], kv.at[m, slot(1, piece)], fsend.at[0], srecv.at[0, k],
            device_id={"sp": i - 1},
        )

    odd = lax.rem(i, 2) == 1

    def sends(b):
        return (i + b < s) & jnp.logical_not(odd) if b == 1 else i + b < s

    def finish(m, piece):
        part = rows_of(piece)
        total = own[m, part]
        for o in range(1, chips):
            psendcopy(o, m, piece).wait_recv()
            total = total + pr[o - 1, m, part].astype(jnp.float32)
        kv[m, slot(0, piece), :] = total.astype(jnp.bfloat16)
        for b in range(reach, 0, -1):
            @pl.when(sends(b))
            def _():
                shiftcopy(b, m, piece).start()

    def pass_on(m, piece):
        @pl.when(i >= 2)
        def _():
            shiftcopy(2, m, piece).wait_recv()

        @pl.when(odd & (i >= 3))
        def _():
            relay(m, piece).start()

    def arrive(m, piece):
        for b in range(1, reach + 1):
            if b != 2:
                @pl.when(i >= b)
                def _():
                    shiftcopy(b, m, piece).wait_recv()

    factor = HD ** (-0.5) * math.log2(math.e)
    ratio = QH // KVH

    def outcopy(g, u):
        block = (
            pl.ds(u * QB, QB), pl.ds(aligned(g * ratio * HD, ratio * HD), ratio * HD)
        )
        return pltpu.make_async_copy(res.at[block], out.at[block], osem.at[0])

    def attend(g, u):
        base = aligned(g * ratio * HD, HD)
        left = jnp.concatenate(
            [q[u * QB:(u + 1) * QB, pl.ds(base + r * HD, HD)] for r in range(ratio)], 0
        )
        keys = kv[2 * g, u * QB:u * QB + width, :]
        values = kv[2 * g + 1, u * QB:u * QB + width, :]
        scores = lax.dot_general(
            left, keys, (((1,), (1,)), ((), ())), preferred_element_type=jnp.float32
        )
        scores = scores.reshape(ratio, QB, width) + mask[u][None]
        scores = scores.reshape(ratio * QB, width)
        highest = jnp.max(scores, axis=-1, keepdims=True)
        probs = jnp.exp2((scores - highest) * factor)
        total = jnp.sum(probs, axis=-1, keepdims=True)
        result = jnp.dot(
            probs.astype(jnp.bfloat16), values, preferred_element_type=jnp.float32
        )
        result = (result / total).astype(jnp.bfloat16)
        for r in range(ratio):
            res[u * QB:(u + 1) * QB, pl.ds(base + r * HD, HD)] = result[
                r * QB:(r + 1) * QB
            ]
        outcopy(g, u).start()

    def when(condition, action):
        @pl.when(condition)
        def _():
            action()

    def cuts(m):
        if m < SPLIT:
            return (EARLY, LATE)
        return (FIRST, SECOND) if m >= LAST else (None,)

    def finish_all(messages, piece):
        for m in messages:
            finish(m, piece)

    def pass_all(messages, piece):
        for m in messages:
            pass_on(m, piece)

    def first_rest():
        if give:
            for h in range(1, parts):
                for o in range(lines):
                    inward(h, o)
            gathered(0)
            for j in range(PAIRS // parts):
                own_rest(j)

    def later_rest():
        if give:
            for h in range(1, parts):
                gathered(h)
                for j in range(PAIRS // parts * h, PAIRS // parts * (h + 1)):
                    own_rest(j)

    def give_all(j, piece):
        for o in range(1, chips):
            give_back(o, j, piece)

    for o in range(1, chips):
        take(xrecv.at[o - 1, 0], xr.at[o - 1, rows_of(EARLY)])
        give_back(o, 0, EARLY)
    first_rest()
    for o in range(1, chips):
        take(xrecv.at[o - 1, 1], xr.at[o - 1, rows_of(LATE)])
        give_back(o, 0, LATE)
    for j in range(1, PAIRS):
        give_all(j, None)
        finish(j - 1, EARLY)
    later_rest()
    finish(SPLIT - 1, EARLY)
    finish_all(range(SPLIT), LATE)
    pass_all(range(SPLIT), EARLY)
    finish(SPLIT, None)
    pass_all(range(SPLIT), LATE)

    def serve(k, lead, relays):
        if k + lead < MSGS:
            for cut in cuts(k + lead):
                finish(k + lead, cut)
        if relays and SPLIT <= k + lead - 3 < MSGS:
            for cut in cuts(k + lead - 3):
                pass_on(k + lead - 3, cut)

    when(i >= 2, lambda: finish_all(range(SPLIT + 1, LEAD), None))

    def ready(g):
        for m in (2 * g, 2 * g + 1):
            for cut in cuts(m):
                arrive(m, cut)

    for g in range(KVH):
        for u in range(tokens // QB):
            k = g * (tokens // QB) + u
            when(i >= 2, functools.partial(serve, k, LEAD, True))
            when(i < 2, functools.partial(serve, k, NEAR, False))
            if u == 0:
                ready(g)
            attend(g, u)

    for o in range(1, chips):
        take(xsend.at[o - 1], xr.at[o - 1])
        take(psend.at[o - 1], ps.at[o - 1])
    for b in range(1, reach + 1):
        when(sends(b), functools.partial(take, ssend.at[b - 1], kv.at[:, slot(0, None)]))
    when(odd & (i >= 3), functools.partial(take, fsend.at[0], kv.at[:, slot(2, None)]))
    if give:
        regain()
    pltpu.make_async_copy(res, out, osem.at[0]).wait()


def shards(n, s, hidden, queries, norm_gain, kv_weight, value_bias, doc_lengths):
    _, tokens, depth = hidden.shape
    reach = s // 4
    chips = n // 2
    rows = kv_weight.shape[0]
    far = chips - 1
    give = rows * SHARE // 10 // HD * HD if chips == 2 and s % 2 == 0 else 0
    if give % (16 * s):
        give = 0
    kept = rows - give
    vmem = pltpu.VMEM
    dma = pltpu.SemaphoreType.DMA
    taken = [
        vmem((PARTS, 2 * give, 2 * KVH * HD // PARTS), jnp.bfloat16),
        dma((PARTS,)),
        dma((PARTS,)),
        dma((PARTS, 2)),
        dma((PARTS,)),
        dma((PARTS, s)),
        dma((PARTS,)),
        dma((PARTS,)),
    ] if give else []
    hold = lambda a: pltpu.with_memory_space_constraint(a, pltpu.HBM)
    anywhere = pl.BlockSpec(memory_space=pltpu.HBM)
    result = pl.pallas_call(
        functools.partial(kernel, n, s, reach, give),
        out_shape=jax.ShapeDtypeStruct((tokens, QH * HD), jnp.bfloat16),
        in_specs=[anywhere] * 6,
        out_specs=anywhere,
        scratch_shapes=[
            pltpu.SMEM((1, doc_lengths.shape[1]), jnp.int32),
            vmem((tokens, depth), jnp.bfloat16),
            vmem((tokens, QH * HD), jnp.bfloat16),
            vmem((tokens, QH * HD), jnp.bfloat16),
            vmem((1, depth + 8 * HD), jnp.float32),
            vmem((1, KVH * HD), jnp.float32),
            vmem((2 * rows, 2 * KVH * HD), jnp.bfloat16),
            vmem((chips, tokens, 2 * rows), jnp.bfloat16),
            vmem((far, tokens, 2 * kept), jnp.bfloat16),
            vmem((MSGS, tokens, HD), jnp.float32),
            vmem((far, MSGS, tokens, HD), jnp.bfloat16),
            vmem((far, MSGS, tokens, HD), jnp.bfloat16),
            vmem((MSGS, (reach + 1) * tokens, HD), jnp.bfloat16),
            vmem((tokens // QB, QB, reach * tokens + QB), jnp.float32),
            dma((6,)),
            dma((XCH,)),
            dma((2, 2)),
            dma((far,)),
            dma((far, 2)),
            dma((far,)),
            dma((far, SEATS)),
            dma((reach,)),
            dma((reach, SEATS)),
            dma((1,)),
            dma((1,)),
        ] + taken,
        compiler_params=pltpu.CompilerParams(
            collective_id=0, has_side_effects=True, vmem_limit_bytes=50 * 1024 * 1024
        ),
    )(
        hidden[0], queries[0], hold(norm_gain.reshape(1, depth)), kv_weight,
        hold(value_bias.reshape(1, KVH * HD)), hold(doc_lengths),
    )
    return result.reshape(1, tokens, QH * HD)


def solution(mesh):
    in_specs = (
        P("fsdp", "sp", None),
        P("fsdp", "sp", None),
        P(),
        P("fsdp", None),
        P(),
        P("fsdp", None),
    )
    body = functools.partial(shards, mesh.shape["fsdp"], mesh.shape["sp"])
    return jax.shard_map(
        body, mesh=mesh, in_specs=in_specs, out_specs=P("fsdp", "sp", None), check_vma=False
    )
```

```python
import functools
import math

import jax
import jax.numpy as jnp
from jax import lax
from jax.experimental import pallas as pl
from jax.experimental.pallas import tpu as pltpu
from jax.sharding import PartitionSpec as P

QH = 32
KVH = 8
HD = 128
EPS = 1e-06
PAIR = 2 * HD
PAIRS = KVH // 2
MSGS = 2 * KVH
LAST = MSGS - 2
SPLIT = 4
LEAD = 6
NEAR = 5
SEATS = 2 * MSGS
HALVED = 4
FIRST, SECOND, EARLY, LATE = range(4)
XCH = 8
QB = 128
MASKED = -1e30
SHARE = 3
PARTS = 2


def aligned(index, step):
    return index if isinstance(index, int) else pl.multiple_of(index, step)


def kernel(
    n, s, reach, give,
    x_hbm, q_hbm, gain_hbm, w_hbm, vbias_hbm, docs_hbm,
    out,
    docs, x, q, res, gain, vbias, w, xs, xr, own, ps, pr, kv, mask,
    local_sem, x_sem, wsem, xsend, xrecv, psend, precv, ssend, srecv, arrived, fsend, osem,
    *gather,
):
    tokens, depth = x.shape
    chips = n // 2
    rows = w_hbm.shape[0]
    half = 2 * rows
    kept = rows - give
    sent = 2 * kept
    mine = lax.axis_index("fsdp")
    i = lax.axis_index("sp")
    core = lax.rem(mine, 2)
    chip = mine // 2
    mate = chip * 2 + (1 - core)
    step = tokens // XCH

    barrier = pltpu.get_barrier_semaphore()
    pl.semaphore_signal(barrier, inc=1, device_id={"fsdp": mate})
    for o in range(1, chips):
        peer = lax.rem(chip + o, chips) * 2 + core
        pl.semaphore_signal(barrier, inc=1, device_id={"fsdp": peer})
    if give:
        for o in range(1, s):
            pl.semaphore_signal(barrier, inc=1, device_id={"sp": lax.rem(i + o, s)})
        callers = chips + s - 1
    else:
        for b in range(1, reach + 1):
            @pl.when(i >= b)
            def _():
                pl.semaphore_signal(barrier, inc=1, device_id={"sp": i - b})

            @pl.when(i + b < s)
            def _():
                pl.semaphore_signal(barrier, inc=1, device_id={"sp": i + b})
        callers = chips + jnp.minimum(i, reach) + jnp.minimum(s - 1 - i, reach)

    def take(sem, ref):
        pltpu.make_async_copy(ref, ref, sem).wait()

    def xcopy(c):
        part = pl.ds(c * step, step)
        return pltpu.make_async_copy(x_hbm.at[part], x.at[part], x_sem.at[c])

    gcopy = pltpu.make_async_copy(gain_hbm, gain.at[:, pl.ds(0, depth)], local_sem.at[0])
    gcopy.start()
    dcopy = pltpu.make_async_copy(docs_hbm, docs, local_sem.at[4])
    dcopy.start()
    for c in range(XCH):
        xcopy(c).start()
    qcopy = pltpu.make_async_copy(q_hbm, q, local_sem.at[2])
    bcopy = pltpu.make_async_copy(vbias_hbm, vbias, local_sem.at[3])

    bands = [(pl.ds(give, kept), pl.ds(core * kept, kept))]
    if give:
        bands.append((pl.ds(0, give), pl.ds(sent + core * give, give)))

    def wcopies():
        return [
            pltpu.make_async_copy(w_hbm.at[a], w.at[b], local_sem.at[(1, 5)[k]])
            for k, (a, b) in enumerate(bands)
        ]

    def wsends():
        return [
            pltpu.make_async_remote_copy(
                w_hbm.at[a], w.at[b], wsem.at[k, 0], wsem.at[k, 1], device_id={"fsdp": mate}
            )
            for k, (a, b) in enumerate(bands)
        ]

    def xsendcopy(o, c):
        target = lax.rem(chip + o, chips)
        part = pl.ds(c * step, step)
        return pltpu.make_async_remote_copy(
            xs.at[target, part, pl.ds(0, sent)], xr.at[o - 1, part], xsend.at[o - 1],
            xrecv.at[o - 1, c // (XCH - 2)], device_id={"fsdp": target * 2 + core},
        )

    if give:
        wg, ysend, yrecv, zsend, hsend, grecv, msend, mrecv = gather
        parts, _, wide_cols = wg.shape
        strip = give // s
        lines = s // 2
        beside = i + 1 - 2 * lax.rem(i, 2)

        def slab(c, k):
            return pl.ds(pl.multiple_of(c * give + k * strip, 16), strip)

        def ygive(h, kind):
            span = wide_cols // 2
            return pltpu.make_async_remote_copy(
                w_hbm.at[pl.ds(pl.multiple_of(i * strip, 16), strip),
                         pl.ds(kind * (KVH * HD) + h * span, span)],
                wg.at[h, slab(core, i), pl.ds(kind * span, span)],
                ysend.at[h], yrecv.at[h],
                device_id={"fsdp": (1 - chip) * 2 + core},
            )

        def zgive(h, k, up):
            return pltpu.make_async_remote_copy(
                wg.at[h, slab(core, k)], wg.at[h, slab(core, k)], zsend.at[h, up],
                grecv.at[h, k], device_id={"sp": i + (2 if up else -2)},
            )

        def has(up):
            return i + 2 < s if up else i >= 2

        def hgive(h, k):
            return pltpu.make_async_remote_copy(
                wg.at[h, slab(core, k)], wg.at[h, slab(core, k)], hsend.at[h],
                grecv.at[h, k], device_id={"sp": beside},
            )

        def mgive(h, k, c):
            return pltpu.make_async_remote_copy(
                wg.at[h, slab(c, k)], wg.at[h, slab(c, k)], msend.at[h], mrecv.at[h],
                device_id={"fsdp": mate},
            )

        def spread(h):
            take(yrecv.at[h], wg.at[h, slab(core, i)])
            for up in (1, 0):
                @pl.when(has(up))
                def _():
                    zgive(h, i, up).start()
            hgive(h, i).start()
            mgive(h, i, core).start()

        def across(h, d):
            for up in (1, 0):
                k = i - 2 * d if up else i + 2 * d

                @pl.when(k >= 0 if up else k < s)
                def _():
                    hgive(h, k).wait_recv()

                    @pl.when(has(up))
                    def _():
                        zgive(h, k, up).start()

                    hgive(h, k).start()
                    mgive(h, k, core).start()

        def inward(h, o):
            k = lax.rem(beside + s - 2 * o, s)
            hgive(h, k).wait_recv()
            mgive(h, k, core).start()

        def gathered(h):
            take(mrecv.at[h], wg.at[h, pl.ds(pl.multiple_of((1 - core) * give, 16), give)])

        def regain():
            for h in range(parts):
                take(ysend.at[h], wg.at[h, pl.ds(0, strip)])
                take(hsend.at[h], wg.at[h, pl.ds(0, lines * strip)])
                take(msend.at[h], wg.at[h, pl.ds(0, give)])
                for up in (1, 0):
                    for d in range(lines - 1):
                        passed = i // 2 if up else lines - 1 - i // 2

                        @pl.when(passed == d)
                        def _():
                            take(zsend.at[h, up], wg.at[h, pl.ds(0, (d + 1) * strip)])

    pieces_of = [(0, give, kept), (kept, rows + give, kept)]
    if give:
        pieces_of += [(sent, 0, give), (sent + give, rows, give)]
    gcopy.wait()
    dcopy.wait()
    for c in range(XCH):
        xcopy(c).wait()
        part = slice(c * step, (c + 1) * step)
        wide = x[part, :].astype(jnp.float32)
        inv = lax.rsqrt(jnp.mean(wide * wide, axis=-1, keepdims=True) + EPS)
        for t in range(chips):
            for to, at, size in pieces_of:
                cut = slice(t * half + at, t * half + at + size)
                piece = x[part, cut].astype(jnp.float32) * inv * gain[:, cut]
                xs[t, part, to:to + size] = piece.astype(jnp.bfloat16)
        if c == 0:
            pl.semaphore_wait(barrier, callers)
            if give:
                for h in range(parts):
                    for kind in range(2):
                        ygive(h, kind).start()
        for o in range(1, chips):
            xsendcopy(o, c).start()
        if c == 0:
            for copy in wsends() + wcopies():
                copy.start()
            bcopy.start()
            qcopy.start()

    first = i * tokens
    width = reach * tokens + QB
    for u in range(tokens // QB):
        pos = first + u * QB + lax.broadcasted_iota(jnp.int32, (QB, 1), 0)
        start = jnp.zeros((QB, 1), jnp.int32)
        end = jnp.int32(0)
        for d in range(docs.shape[1]):
            end = end + docs[0, d]
            start = jnp.where(pos >= end, end, start)
        key = first + u * QB - reach * tokens + lax.broadcasted_iota(jnp.int32, (QB, width), 1)
        mask[u] = jnp.where((key >= start) & (key <= pos), 0.0, MASKED)
    for b in range(1, reach + 1):
        @pl.when(i < b)
        def _():
            kv[:, (reach - b) * tokens:(reach - b + 1) * tokens, :] = jnp.zeros(
                (MSGS, tokens, HD), jnp.bfloat16
            )

    def project(left, right, j, kind):
        cols = pl.ds(aligned(kind * (KVH * HD) + j * PAIR, PAIR), PAIR)
        return jnp.dot(left[...], right[:, cols], preferred_element_type=jnp.float32)

    if give:
        for h in range(parts):
            spread(h)
        across(0, 1)
    for copy in wcopies():
        copy.wait()
    for copy in wsends():
        copy.wait()
    bcopy.wait()
    qcopy.wait()

    def own_pair(j):
        keys = project(xs.at[chip], w, j, 0)
        values = project(xs.at[chip], w, j, 1)
        values = values + vbias[:, pl.ds(aligned(j * PAIR, PAIR), PAIR)]
        for h in range(2):
            own[4 * j + 2 * h] = keys[:, h * HD:(h + 1) * HD]
            own[4 * j + 2 * h + 1] = values[:, h * HD:(h + 1) * HD]

    def own_rest(j):
        left = xs[1 - chip, :, sent:]
        group = PAIRS // parts
        h = j // group
        for kind in range(2):
            cols = pl.ds((kind * group + j % group) * PAIR, PAIR)
            more = jnp.dot(left, wg[h, :, cols], preferred_element_type=jnp.float32)
            for r in range(2):
                own[4 * j + 2 * r + kind] += more[:, r * HD:(r + 1) * HD]

    if give:
        turns = [(h, d) for d in range(1, lines) for h in range(parts)][1:]
        for j in range(PAIRS):
            own_pair(j)
            for turn in turns[j:j + 1]:
                across(*turn)
        for turn in turns[PAIRS:]:
            across(*turn)
        for o in range(lines):
            inward(0, o)
    else:
        @pl.loop(0, PAIRS)
        def _(j):
            own_pair(j)

    half_tokens = tokens // 2
    ahead = (XCH - 2) * step
    spans = {
        None: (0, tokens),
        FIRST: (0, half_tokens),
        SECOND: (half_tokens, half_tokens),
        EARLY: (0, ahead),
        LATE: (ahead, tokens - ahead),
    }

    def cuts(m):
        if m < SPLIT:
            return (EARLY, LATE)
        return (FIRST, SECOND) if m >= HALVED else (None,)

    def rows_of(piece):
        return pl.ds(*spans[piece])

    def seat(m, piece):
        return m + (MSGS if piece in (SECOND, LATE) else 0)

    def psendcopy(o, m, piece):
        source = lax.rem(chip + chips - o, chips)
        k = seat(m, piece)
        return pltpu.make_async_remote_copy(
            ps.at[o - 1, m, rows_of(piece)], pr.at[o - 1, m, rows_of(piece)],
            psend.at[o - 1], precv.at[o - 1, k], device_id={"fsdp": source * 2 + core},
        )

    def give_back(o, j, piece):
        part = rows_of(piece)
        for kind in range(2):
            partial = project(
                xr.at[o - 1, part], w.at[pl.ds(0, sent)], j, kind
            ).astype(jnp.bfloat16)
            for h in range(2):
                ps[o - 1, 4 * j + 2 * h + kind, part, :] = partial[:, h * HD:(h + 1) * HD]
        for m in range(4 * j, 4 * j + 4):
            for cut in (piece,) if m < SPLIT else cuts(m):
                psendcopy(o, m, cut).start()

    def slot(b, piece):
        start, size = spans[piece]
        return pl.ds((reach - b) * tokens + start, size)

    def shiftcopy(b, m, piece):
        k = seat(m, piece)
        return pltpu.make_async_remote_copy(
            kv.at[m, slot(0, piece)], kv.at[m, slot(b, piece)], ssend.at[b - 1],
            srecv.at[k] if b == 2 else arrived.at[max(b - 2, 0), m // 2], device_id={"sp": i + b},
        )

    def relay(m, piece):
        k = seat(m, piece)
        return pltpu.make_async_remote_copy(
            kv.at[m, slot(2, piece)], kv.at[m, slot(1, piece)], fsend.at[0],
            arrived.at[0, m // 2],
            device_id={"sp": i - 1},
        )

    odd = lax.rem(i, 2) == 1

    def sends(b):
        return (i + b < s) & jnp.logical_not(odd) if b == 1 else i + b < s

    def finish(m, piece):
        part = rows_of(piece)
        total = own[m, part]
        for o in range(1, chips):
            psendcopy(o, m, piece).wait_recv()
            total = total + pr[o - 1, m, part].astype(jnp.float32)
        kv[m, slot(0, piece), :] = total.astype(jnp.bfloat16)
        for b in range(reach, 0, -1):
            @pl.when(sends(b))
            def _():
                shiftcopy(b, m, piece).start()

    def pass_on(m, piece):
        @pl.when(i >= 2)
        def _():
            shiftcopy(2, m, piece).wait_recv()

        @pl.when(odd & (i >= 3))
        def _():
            relay(m, piece).start()

    def arrive(g):
        for b in range(1, reach + 1):
            if b != 2:
                @pl.when(i >= b)
                def _():
                    take(arrived.at[max(b - 2, 0), g], kv.at[pl.ds(2 * g, 2), slot(b, None)])

    factor = HD ** (-0.5) * math.log2(math.e)
    ratio = QH // KVH

    def outcopy(g, u):
        block = (
            pl.ds(u * QB, QB), pl.ds(aligned(g * ratio * HD, ratio * HD), ratio * HD)
        )
        return pltpu.make_async_copy(res.at[block], out.at[block], osem.at[0])

    def attend(g, u):
        base = aligned(g * ratio * HD, HD)
        left = jnp.concatenate(
            [q[u * QB:(u + 1) * QB, pl.ds(base + r * HD, HD)] for r in range(ratio)], 0
        )
        keys = kv[2 * g, u * QB:u * QB + width, :]
        values = kv[2 * g + 1, u * QB:u * QB + width, :]
        scores = lax.dot_general(
            left, keys, (((1,), (1,)), ((), ())), preferred_element_type=jnp.float32
        )
        scores = scores.reshape(ratio, QB, width) + mask[u][None]
        scores = scores.reshape(ratio * QB, width)
        highest = jnp.max(scores, axis=-1, keepdims=True)
        probs = jnp.exp2((scores - highest) * factor)
        total = jnp.sum(probs, axis=-1, keepdims=True)
        result = jnp.dot(
            probs.astype(jnp.bfloat16), values, preferred_element_type=jnp.float32
        )
        result = (result / total).astype(jnp.bfloat16)
        for r in range(ratio):
            res[u * QB:(u + 1) * QB, pl.ds(base + r * HD, HD)] = result[
                r * QB:(r + 1) * QB
            ]
        outcopy(g, u).start()

    def when(condition, action):
        @pl.when(condition)
        def _():
            action()

    def finish_all(messages, piece):
        for m in messages:
            finish(m, piece)

    def pass_all(messages, piece):
        for m in messages:
            pass_on(m, piece)

    def first_rest():
        if give:
            for h in range(1, parts):
                for o in range(lines):
                    inward(h, o)
            gathered(0)
            for j in range(PAIRS // parts):
                own_rest(j)

    def later_rest():
        if give:
            for h in range(1, parts):
                gathered(h)
                for j in range(PAIRS // parts * h, PAIRS // parts * (h + 1)):
                    own_rest(j)

    def give_all(j, piece):
        for o in range(1, chips):
            give_back(o, j, piece)

    for o in range(1, chips):
        take(xrecv.at[o - 1, 0], xr.at[o - 1, rows_of(EARLY)])
        give_back(o, 0, EARLY)
    first_rest()
    for o in range(1, chips):
        take(xrecv.at[o - 1, 1], xr.at[o - 1, rows_of(LATE)])
        give_back(o, 0, LATE)
    for j in range(1, PAIRS):
        give_all(j, None)
        finish(j - 1, EARLY)
    later_rest()
    finish(SPLIT - 1, EARLY)
    finish_all(range(SPLIT), LATE)
    pass_all(range(SPLIT), EARLY)
    for cut in cuts(SPLIT):
        finish(SPLIT, cut)
    pass_all(range(SPLIT), LATE)

    def serve(k, lead, relays):
        for turn in range(2):
            m = k + lead
            if m < MSGS:
                for cut in cuts(m)[turn:turn + 1]:
                    finish(m, cut)
            m = m - 3
            if relays and SPLIT <= m < MSGS:
                for cut in cuts(m)[turn:turn + 1]:
                    pass_on(m, cut)

    def start(lead):
        for m in range(SPLIT + 1, lead):
            for cut in cuts(m):
                finish(m, cut)

    when(i >= 2, functools.partial(start, LEAD))

    for g in range(KVH):
        for u in range(tokens // QB):
            k = g * (tokens // QB) + u
            when(i >= 2, functools.partial(serve, k, LEAD, True))
            when(i < 2, functools.partial(serve, k, NEAR, False))
            if u == 0:
                arrive(g)
            attend(g, u)

    for o in range(1, chips):
        take(xsend.at[o - 1], xr.at[o - 1])
        take(psend.at[o - 1], ps.at[o - 1])
    for b in range(1, reach + 1):
        when(sends(b), functools.partial(take, ssend.at[b - 1], kv.at[:, slot(0, None)]))
    when(odd & (i >= 3), functools.partial(take, fsend.at[0], kv.at[:, slot(2, None)]))
    if give:
        regain()
    pltpu.make_async_copy(res, out, osem.at[0]).wait()


def shards(n, s, hidden, queries, norm_gain, kv_weight, value_bias, doc_lengths):
    _, tokens, depth = hidden.shape
    reach = s // 4
    chips = n // 2
    rows = kv_weight.shape[0]
    far = chips - 1
    give = rows * SHARE // 10 // HD * HD if chips == 2 and s % 2 == 0 else 0
    if give % (16 * s):
        give = 0
    kept = rows - give
    vmem = pltpu.VMEM
    dma = pltpu.SemaphoreType.DMA
    taken = [
        vmem((PARTS, 2 * give, 2 * KVH * HD // PARTS), jnp.bfloat16),
        dma((PARTS,)),
        dma((PARTS,)),
        dma((PARTS, 2)),
        dma((PARTS,)),
        dma((PARTS, s)),
        dma((PARTS,)),
        dma((PARTS,)),
    ] if give else []
    hold = lambda a: pltpu.with_memory_space_constraint(a, pltpu.HBM)
    anywhere = pl.BlockSpec(memory_space=pltpu.HBM)
    result = pl.pallas_call(
        functools.partial(kernel, n, s, reach, give),
        out_shape=jax.ShapeDtypeStruct((tokens, QH * HD), jnp.bfloat16),
        in_specs=[anywhere] * 6,
        out_specs=anywhere,
        scratch_shapes=[
            pltpu.SMEM((1, doc_lengths.shape[1]), jnp.int32),
            vmem((tokens, depth), jnp.bfloat16),
            vmem((tokens, QH * HD), jnp.bfloat16),
            vmem((tokens, QH * HD), jnp.bfloat16),
            vmem((1, depth + 8 * HD), jnp.float32),
            vmem((1, KVH * HD), jnp.float32),
            vmem((2 * rows, 2 * KVH * HD), jnp.bfloat16),
            vmem((chips, tokens, 2 * rows), jnp.bfloat16),
            vmem((far, tokens, 2 * kept), jnp.bfloat16),
            vmem((MSGS, tokens, HD), jnp.float32),
            vmem((far, MSGS, tokens, HD), jnp.bfloat16),
            vmem((far, MSGS, tokens, HD), jnp.bfloat16),
            vmem((MSGS, (reach + 1) * tokens, HD), jnp.bfloat16),
            vmem((tokens // QB, QB, reach * tokens + QB), jnp.float32),
            dma((6,)),
            dma((XCH,)),
            dma((2, 2)),
            dma((far,)),
            dma((far, 2)),
            dma((far,)),
            dma((far, SEATS)),
            dma((reach,)),
            dma((SEATS,)),
            dma((max(reach - 1, 1), KVH)),
            dma((1,)),
            dma((1,)),
        ] + taken,
        compiler_params=pltpu.CompilerParams(
            collective_id=0, has_side_effects=True, vmem_limit_bytes=50 * 1024 * 1024
        ),
    )(
        hidden[0], queries[0], hold(norm_gain.reshape(1, depth)), kv_weight,
        hold(value_bias.reshape(1, KVH * HD)), hold(doc_lengths),
    )
    return result.reshape(1, tokens, QH * HD)


def solution(mesh):
    in_specs = (
        P("fsdp", "sp", None),
        P("fsdp", "sp", None),
        P(),
        P("fsdp", None),
        P(),
        P("fsdp", None),
    )
    body = functools.partial(shards, mesh.shape["fsdp"], mesh.shape["sp"])
    return jax.shard_map(
        body, mesh=mesh, in_specs=in_specs, out_specs=P("fsdp", "sp", None), check_vma=False
    )
```
